128 devices in a mesh: groups: 4 (over x, y), expert: 2 (over core), seq: 16 (over z).
Axes of the slice: x: 2, y: 2, z: 16, core: 2. Of those that a mesh axis runs over, the one named last changes fastest.
The devices are a block of a 8x8x16 slice.
Arguments:
- query_heads: bfloat16 [2, 4, 2080, 4096], P('expert', 'groups', 'seq'), parts along dimension 1, may hold values from -100 to 100
- key_heads: bfloat16 [2, 4, 2080, 4096], P('expert', 'groups', 'seq'), parts along dimension 1, may hold values from -8 to 8
- value_heads: bfloat16 [2, 4, 2080, 4096], P('expert', 'groups', 'seq'), parts along dimension 1, may hold values from -6 to 6
- residual: bfloat16 [2, 4, 2080, 5120], P('expert', 'groups', 'seq'), parts along dimension 1, may hold values from -6 to 6
- out_weight: bfloat16 [2, 4096, 5120], P('expert', 'seq'), may hold values from -0.09375 to 0.09375
- mod_weight: bfloat16 [2, 256, 15360], P('expert'), may hold values from -0.375 to 0.375
- head_weight: bfloat16 [2, 5120, 64], P('expert'), may hold values from -0.078125 to 0.078125
- latent: float32 [4, 2080, 64], P('groups', 'seq'), parts along dimension 0, may hold values from -6 to 6
- timesteps: int32 [2, 4], P('expert', 'groups'), parts along dimension 1, may hold values from 26 to 1000, as said below
- token_order: int32 [2, 4, 2080], P(None, 'groups'), parts along dimension 1, may hold values from 0 to 2079, as said below
Outputs:
- velocity: float32 [2, 4, 2080, 64], P('expert', 'groups', 'seq'), parts along dimension 1
- latents_out: float32 [2, 4, 2080, 64], P('expert', 'groups', 'seq'), parts along dimension 1
The draws below stay inside these ranges and needn't reach their ends.
There are 4 independent parts, one for each index of `groups`. The reference program is written for one: setup_inputs(seed, part) draws one part's arguments, and reference() takes and returns one part's arrays. A program takes and returns all parts, laid end to end along the dimension named above; an argument that names none is the same for every part. Nothing has to cross between parts.
Inputs may be any that keep to these rules, and one draw needn't show every extreme that they name: Each token_order[e, m] is a permutation of 0 to 2079. timesteps[0, m] is at least 876 and timesteps[1, m] at most 875.
All inputs are finite; a program needn't handle non-finite values.
Results may differ from the reference program's by a relative error of at most 0.0085.
Values may be sent and summed in bfloat16 or wider, within the bound.
No kernel may reach another device: no remote copies, remote signals or barrier semaphores. Data moves between devices by JAX's collectives and lax.ppermute only.
A program may use at most 128 MiB of HBM per device.

```python
import jax
import jax.numpy as jnp
from jax import lax

D = 5120
HEAD_DIM = 128
FREQ = 256
LATENT = 64
HEADS = 32
HGRID = 20
WGRID = 52
MB = 1
STRIDE = 25
L = 2080


def token_orders(key):
    streams = jax.random.split(jax.random.fold_in(key, 4099), 2 * MB)
    shuffled = jax.vmap(lambda stream: jax.random.permutation(stream, L))(streams)
    return shuffled.reshape(2, MB, L).astype(jnp.int32)


def drawn_fields(key):
    first_key, second_key = jax.random.split(jax.random.fold_in(key, 5003))
    field_shape = (2, MB, L, HEADS, HEAD_DIM)
    queries = jnp.clip(jax.random.normal(first_key, field_shape), -4.0, 4.0)
    keys_out = jnp.clip(jax.random.normal(second_key, field_shape), -4.0, 4.0)
    return (queries, keys_out)


def draw_query_heads(key, part):
    return drawn_fields(key)[0].reshape(2, MB, L, HEADS * HEAD_DIM).astype(jnp.bfloat16)


def draw_key_heads(key, part):
    return drawn_fields(key)[1].reshape(2, MB, L, HEADS * HEAD_DIM).astype(jnp.bfloat16)


def draw_residual(key, part):
    split_keys = jax.random.split(jax.random.fold_in(key, 9001), 1)
    field = 0.03 * jax.random.normal(split_keys[0], (2, MB, L, D))
    return field.astype(jnp.bfloat16)


def draw_timesteps(key, part):
    early_key, late_key = jax.random.split(jax.random.fold_in(key, 8191))
    upper_steps = jax.random.randint(early_key, (1, MB), 876, 1001)
    lower_steps = jax.random.randint(late_key, (1, MB), 26, 876)
    return jnp.concatenate([upper_steps, lower_steps], axis=0).astype(jnp.int32)


def draw_token_order(key, part):
    return token_orders(key)


def shard_levels(stream_key, extent, shards, least, top_value):
    gain, own = 1.0, jax.random.fold_in(stream_key, 6)
    for position, shards_of in shards:
        steps = jnp.exp(jax.random.uniform(jax.random.fold_in(own, position), (shards_of,), jnp.float32, least / len(shards), top_value / len(shards)))
        gain = gain * jnp.repeat(steps, extent[position] // shards_of).reshape([-1 if axis == position else 1 for axis in range(len(extent))])
    return gain


def noise(own_key, dims, width, limit, cuts=(), held_as=jnp.bfloat16):
    level = shard_levels(own_key, dims, cuts, -0.22, 0.18) if cuts else 1.0
    entries = jax.random.normal(own_key, dims, jnp.float32) * width * level
    return jnp.minimum(jnp.maximum(entries, -limit), limit).astype(held_as)


def setup_inputs(seed: int = 0, part: int = 0) -> dict:
    seeds = jax.random.split(jax.random.key(seed), 11)
    own_keys = jax.random.split(jax.random.fold_in(seeds[10], part), 11)
    query_heads = draw_query_heads(jax.random.fold_in(jax.random.fold_in(seeds[10], part), 71), part)
    key_heads = draw_key_heads(jax.random.fold_in(jax.random.fold_in(seeds[10], part), 71), part)
    value_heads = noise(own_keys[2], (2, MB, L, HEADS * HEAD_DIM), 1.0, 6.0, ((0, 2), (2, 16)))
    residual = draw_residual(jax.random.fold_in(jax.random.fold_in(seeds[10], part), 71), part)
    out_weight = noise(seeds[4], (2, HEADS * HEAD_DIM, D), (HEADS * HEAD_DIM) ** -0.5, 0.09375, ((0, 2), (1, 16)))
    mod_weight = noise(seeds[5], (2, FREQ, 3 * D), FREQ ** -0.5, 0.375, ((0, 2),))
    head_weight = noise(seeds[6], (2, D, LATENT), D ** -0.5, 0.078125, ((0, 2),))
    latent = noise(own_keys[7], (MB, L, LATENT), 1.0, 6.0, ((1, 16),), jnp.float32)
    timesteps = draw_timesteps(jax.random.fold_in(jax.random.fold_in(seeds[10], part), 71), part)
    token_order = draw_token_order(jax.random.fold_in(jax.random.fold_in(seeds[10], part), 71), part)
    return dict(query_heads=query_heads, key_heads=key_heads, value_heads=value_heads, residual=residual, out_weight=out_weight, mod_weight=mod_weight, head_weight=head_weight, latent=latent, timesteps=timesteps, token_order=token_order)


flow_shift = 5.0
norm_eps = 1e-06

def ladder(length):
    return 10000.0 ** (-jnp.arange(length, dtype=jnp.float32) / length)

def rope_angles(tokens):
    half_dim = HEAD_DIM // 2
    side_pairs = half_dim // 3
    frame_pairs = half_dim - 2 * side_pairs
    frame_pos = (tokens // (HGRID * WGRID)).astype(jnp.float32)
    row_pos = (tokens // WGRID % HGRID).astype(jnp.float32)
    column_pos = (tokens % WGRID).astype(jnp.float32)
    return jnp.concatenate([frame_pos[:, None] * ladder(frame_pairs), row_pos[:, None] * ladder(side_pairs), column_pos[:, None] * ladder(side_pairs)], axis=1)

def rotate(field, angles):
    row_count = field.shape[0]
    paired = field.reshape(row_count, -1, HEAD_DIM // 2, 2)
    cosine = jnp.cos(angles)[:, None, :]
    sine_part = jnp.sin(angles)[:, None, :]
    even_part = paired[..., 0]
    odd_part = paired[..., 1]
    turned = jnp.stack([even_part * cosine - odd_part * sine_part, even_part * sine_part + odd_part * cosine], axis=-1)
    return turned.reshape(row_count, -1)

def stamp_embedding(step_value):
    half_freq = FREQ // 2
    inverse_rates = 10000.0 ** (-jnp.arange(half_freq, dtype=jnp.float32) / half_freq)
    phases = step_value * inverse_rates
    return jnp.concatenate([jnp.cos(phases), jnp.sin(phases)])

def noise_level(step_value):
    scaled = step_value / 1000.0
    return flow_shift * scaled / (1.0 + (flow_shift - 1.0) * scaled)

def attend(turned_q, turned_k, values_in):
    split_q = turned_q.reshape(L, HEADS, HEAD_DIM).transpose(1, 0, 2)
    split_k = turned_k.reshape(L, HEADS, HEAD_DIM).transpose(1, 0, 2)
    split_v = values_in.reshape(L, HEADS, HEAD_DIM).transpose(1, 0, 2)

    def one_head(operands):
        head_q, head_k, head_v = operands
        scores = jnp.dot(head_q, head_k.T, preferred_element_type=jnp.float32) * HEAD_DIM ** (-0.5)
        row_max = lax.optimization_barrier(jnp.max(scores, axis=1, keepdims=True))
        weights = jnp.exp(scores - row_max)
        row_total = lax.optimization_barrier(jnp.sum(weights, axis=1, keepdims=True))
        mixed = jnp.dot(weights.astype(jnp.bfloat16), head_v, preferred_element_type=jnp.float32)
        return (mixed / row_total).astype(jnp.bfloat16)
    heads_out = lax.map(one_head, (split_q, split_k, split_v))
    return heads_out.transpose(1, 0, 2).reshape(L, HEADS * HEAD_DIM)

def expert_velocity(queries, keys_in, values_in, residual_rows, out_w, mod_w, head_w, order, step_value):
    angles = rope_angles(order)
    turned_q = rotate(queries.astype(jnp.float32), angles).astype(jnp.bfloat16)
    turned_k = rotate(keys_in.astype(jnp.float32), angles).astype(jnp.bfloat16)
    mixed = attend(turned_q, turned_k, values_in)
    projection = jnp.dot(mixed, out_w, preferred_element_type=jnp.float32)
    embedded = stamp_embedding(step_value).astype(jnp.bfloat16)
    modulation = jnp.dot(embedded[None], mod_w, preferred_element_type=jnp.float32)[0]
    gate_vec = modulation[:D]
    shift_vec = modulation[D:2 * D]
    scale_vec = modulation[2 * D:]
    hidden = residual_rows.astype(jnp.float32) + gate_vec * projection
    centered = hidden - lax.optimization_barrier(jnp.mean(hidden, axis=1, keepdims=True))
    variance = lax.optimization_barrier(jnp.mean(centered * centered, axis=1, keepdims=True))
    normed = (centered * lax.rsqrt(variance + norm_eps) * (1.0 + scale_vec) + shift_vec).astype(jnp.bfloat16)
    return jnp.dot(normed, head_w, preferred_element_type=jnp.float32)

def reference(query_heads, key_heads, value_heads, residual, out_weight, mod_weight, head_weight, latent, timesteps, token_order):
    high_speed, low_speed, high_latent, low_latent = ([], [], [], [])
    for micro_no in range(MB):
        speeds = []
        changes = []
        for expert_no in range(2):
            step_value = timesteps[expert_no, micro_no].astype(jnp.float32)
            speeds.append(expert_velocity(query_heads[expert_no, micro_no], key_heads[expert_no, micro_no], value_heads[expert_no, micro_no], residual[expert_no, micro_no], out_weight[expert_no], mod_weight[expert_no], head_weight[expert_no], token_order[expert_no, micro_no], step_value))
            changes.append(noise_level(step_value - STRIDE) - noise_level(step_value))
        stepped = latent[micro_no] + changes[0] * speeds[0]
        first_order = token_order[0, micro_no]
        inverse = jnp.zeros((L,), jnp.int32).at[first_order].set(jnp.arange(L, dtype=jnp.int32))
        started = stepped[inverse[token_order[1, micro_no]]]
        high_speed.append(speeds[0])
        low_speed.append(speeds[1])
        high_latent.append(stepped)
        low_latent.append(started + changes[1] * speeds[1])
    velocity = jnp.stack([jnp.stack(high_speed), jnp.stack(low_speed)])
    latents_out = jnp.stack([jnp.stack(high_latent), jnp.stack(low_latent)])
    return (velocity, latents_out)
```

```python
import jax
import jax.numpy as jnp
from jax import lax
from jax.experimental import pallas as pl
from jax.experimental.pallas import tpu as pltpu
from jax.sharding import PartitionSpec as P

HEAD_DIM = 128
FREQ = 256
HGRID = 20
WGRID = 52
STRIDE = 25

flow_shift = 5.0
norm_eps = 1e-06


def shift(value, axis, distance):
    n = lax.axis_size(axis)
    return lax.ppermute(value, axis, [(i, (i + distance) % n) for i in range(n)])


def ladder(length):
    return 10000.0 ** (-jnp.arange(length, dtype=jnp.float32) / length)


def rope_tables(tokens):
    half_dim = HEAD_DIM // 2
    side_pairs = half_dim // 3
    frame_pairs = half_dim - 2 * side_pairs
    rates = jnp.repeat(
        jnp.concatenate([ladder(frame_pairs), ladder(side_pairs), ladder(side_pairs)]), 2
    )
    lane = jnp.arange(HEAD_DIM)
    frame_pos = (tokens // (HGRID * WGRID)).astype(jnp.float32)[..., None]
    row_pos = (tokens // WGRID % HGRID).astype(jnp.float32)[..., None]
    column_pos = (tokens % WGRID).astype(jnp.float32)[..., None]
    position = jnp.where(
        lane < 2 * frame_pairs,
        frame_pos,
        jnp.where(lane < 2 * (frame_pairs + side_pairs), row_pos, column_pos),
    )
    angles = position * rates
    sign = jnp.where(lane % 2 == 0, -1.0, 1.0).astype(jnp.float32)
    return jnp.cos(angles), jnp.sin(angles) * sign


def stamp_embedding(step_value):
    half_freq = FREQ // 2
    inverse_rates = 10000.0 ** (-jnp.arange(half_freq, dtype=jnp.float32) / half_freq)
    phases = step_value * inverse_rates
    return jnp.concatenate([jnp.cos(phases), jnp.sin(phases)])


def noise_level(step_value):
    scaled = step_value / 1000.0
    return flow_shift * scaled / (1.0 + (flow_shift - 1.0) * scaled)


def pack_messages(queries, keys, values, seq_index, peers):
    rows, features = queries.shape
    width = features // peers

    def kernel(index_ref, q_ref, k_ref, v_ref, *out_refs):
        base = index_ref[0]
        for d in range(peers):
            owner = lax.rem(base + d, peers)
            at = pl.multiple_of(owner * width, width)
            for part, ref in enumerate((q_ref, k_ref, v_ref)):
                out_refs[d][:, part * width : (part + 1) * width] = ref[:, pl.ds(at, width)]

    vmem = pl.BlockSpec(memory_space=pltpu.VMEM)
    return pl.pallas_call(
        kernel,
        in_specs=[pl.BlockSpec(memory_space=pltpu.SMEM), vmem, vmem, vmem],
        out_specs=[vmem] * peers,
        out_shape=[jax.ShapeDtypeStruct((rows, 3 * width), queries.dtype)] * peers,
        name="pack_messages",
    )(seq_index.reshape(1), queries, keys, values)


def attend(messages, cosine, sine):
    peers = len(messages)
    rows, packed = messages[0].shape
    width = packed // 3
    heads = width // HEAD_DIM
    total = peers * rows
    exponent_scale = HEAD_DIM ** (-0.5) * 1.4426950408889634

    def kernel(*refs):
        message_refs = refs[:peers]
        cos_ref, sin_ref, out_ref, q_scr, k_scr, v_scr = refs[peers:]
        even = lax.broadcasted_iota(jnp.int32, (rows, HEAD_DIM), 1) % 2 == 0
        for d in range(peers):
            cos_d = cos_ref[d]
            sin_d = sin_ref[d]

            def turned(start):
                x = message_refs[d][:, start : start + HEAD_DIM].astype(jnp.float32)
                swapped = jnp.where(even, pltpu.roll(x, HEAD_DIM - 1, 1), pltpu.roll(x, 1, 1))
                return (x * cos_d + swapped * sin_d).astype(jnp.bfloat16)

            for h in range(heads):
                q_scr[d * heads + h] = turned(h * HEAD_DIM)
                k_scr[h, d * rows : (d + 1) * rows, :] = turned(width + h * HEAD_DIM)
                v_at = 2 * width + h * HEAD_DIM
                v_scr[h, d * rows : (d + 1) * rows, :] = message_refs[d][:, v_at : v_at + HEAD_DIM]

        def one_block(d, carry):
            for h in range(heads):
                scores = lax.dot_general(
                    q_scr[d * heads + h],
                    k_scr[h],
                    (((1,), (1,)), ((), ())),
                    preferred_element_type=jnp.float32,
                )
                row_max = jnp.max(scores, axis=1, keepdims=True)
                weights = jnp.exp2((scores - row_max) * exponent_scale)
                row_total = jnp.sum(weights, axis=1, keepdims=True)
                mixed = lax.dot_general(
                    weights.astype(jnp.bfloat16),
                    v_scr[h],
                    (((1,), (0,)), ((), ())),
                    preferred_element_type=jnp.float32,
                )
                out_ref[d, :, h * HEAD_DIM : (h + 1) * HEAD_DIM] = (mixed / row_total).astype(
                    jnp.bfloat16
                )
            return carry

        lax.fori_loop(0, peers, one_block, 0)

    vmem = pl.BlockSpec(memory_space=pltpu.VMEM)
    flops = 4 * total * total * width
    return pl.pallas_call(
        kernel,
        in_specs=[vmem] * (peers + 2),
        out_specs=vmem,
        out_shape=jax.ShapeDtypeStruct((peers, rows, width), jnp.bfloat16),
        scratch_shapes=[
            pltpu.VMEM((peers * heads, rows, HEAD_DIM), jnp.bfloat16),
            pltpu.VMEM((heads, total, HEAD_DIM), jnp.bfloat16),
            pltpu.VMEM((heads, total, HEAD_DIM), jnp.bfloat16),
        ],
        cost_estimate=pl.CostEstimate(
            flops=flops, bytes_accessed=8 * total * width, transcendentals=heads * total * total
        ),
        compiler_params=pltpu.CompilerParams(vmem_limit_bytes=40 * 1024 * 1024),
        name="attend",
    )(*messages, cosine, sine)


def shards(
    query_heads,
    key_heads,
    value_heads,
    residual,
    out_weight,
    mod_weight,
    head_weight,
    latent,
    timesteps,
    token_order,
):
    peers = lax.axis_size("seq")
    seq_index = lax.axis_index("seq")
    expert_index = lax.axis_index("expert")
    block_rows = query_heads.shape[2]
    model_width = residual.shape[3]
    half = model_width // 2

    outgoing = pack_messages(
        query_heads[0, 0], key_heads[0, 0], value_heads[0, 0], seq_index, peers
    )
    arrived = [None] * peers
    arrived[0] = outgoing[0]
    order = [peers // 2]
    for d in range(peers // 2 - 1, 0, -1):
        order += [d, peers - d]
    for d in order:
        arrived[d] = shift(outgoing[d], "seq", d)

    orders = lax.dynamic_index_in_dim(token_order, expert_index, 0, keepdims=False)[0]
    by_device = orders.reshape(peers, block_rows)
    doubled = jnp.concatenate([by_device[::-1], by_device[::-1]], axis=0)
    slot_tokens = lax.dynamic_slice_in_dim(doubled, peers - 1 - seq_index, peers, axis=0)
    own_tokens = slot_tokens[0]
    cosine, sine = rope_tables(slot_tokens)

    step_value = timesteps[0, 0].astype(jnp.float32)
    embedded = stamp_embedding(step_value).astype(jnp.bfloat16)
    modulation = jnp.dot(embedded[None], mod_weight[0], preferred_element_type=jnp.float32)[0]
    gate_vec = modulation[:model_width]
    shift_vec = modulation[model_width : 2 * model_width]
    scale_vec = modulation[2 * model_width :]

    attention = attend(arrived, cosine, sine)

    weight_half = (out_weight[0][:, :half], out_weight[0][:, half:])

    def partial(slot, column_half):
        return jnp.dot(
            attention[slot % peers], weight_half[column_half], preferred_element_type=jnp.float32
        )

    chains = {}
    far = peers // 2
    for way in (1, -1):
        for column_half in (0, 1):
            chains[way, column_half] = None
    chains[1, 0] = shift(partial(far, 0).astype(jnp.bfloat16), "seq", 1)
    chains[-1, 1] = shift(partial(far, 1).astype(jnp.bfloat16), "seq", -1)
    for distance in range(far - 1, 0, -1):
        for key in ((1, 1), (-1, 0), (1, 0), (-1, 1)):
            way, column_half = key
            total = partial(-way * distance, column_half)
            if chains[key] is not None:
                total = total + chains[key].astype(jnp.float32)
            chains[key] = shift(total.astype(jnp.bfloat16), "seq", way)
    projected = jnp.concatenate(
        [
            partial(0, c) + chains[1, c].astype(jnp.float32) + chains[-1, c].astype(jnp.float32)
            for c in (0, 1)
        ],
        axis=1,
    )

    hidden = residual[0, 0].astype(jnp.float32) + gate_vec * projected
    centered = hidden - jnp.mean(hidden, axis=1, keepdims=True)
    variance = jnp.mean(centered * centered, axis=1, keepdims=True)
    normed = (centered * lax.rsqrt(variance + norm_eps) * (1.0 + scale_vec) + shift_vec).astype(
        jnp.bfloat16
    )
    velocity = jnp.dot(normed, head_weight[0], preferred_element_type=jnp.float32)
    change = noise_level(step_value - STRIDE) - noise_level(step_value)
    stepped = latent[0] + change * velocity

    handed = lax.ppermute(stepped.astype(jnp.bfloat16), "expert", [(0, 1)])
    rows = lax.all_gather(handed, "seq", axis=0, tiled=True)
    same_token = (own_tokens[:, None] == token_order[0, 0][None, :]).astype(jnp.bfloat16)
    started = jnp.dot(same_token, rows, preferred_element_type=jnp.float32)
    finished = jnp.where(expert_index == 0, stepped, started + change * velocity)
    return (velocity[None, None], finished[None, None])


def solution(mesh):
    return jax.shard_map(
        shards,
        mesh=mesh,
        in_specs=(
            P("expert", "groups", "seq", None),
            P("expert", "groups", "seq", None),
            P("expert", "groups", "seq", None),
            P("expert", "groups", "seq", None),
            P("expert", "seq", None),
            P("expert", None, None),
            P("expert", None, None),
            P("groups", "seq", None),
            P("expert", "groups"),
            P(None, "groups", None),
        ),
        out_specs=(P("expert", "groups", "seq", None), P("expert", "groups", "seq", None)),
        check_vma=False,
    )
```

```python
import jax
import jax.numpy as jnp
from jax import lax
from jax.experimental import pallas as pl
from jax.experimental.pallas import tpu as pltpu
from jax.sharding import PartitionSpec as P

HEAD_DIM = 128
FREQ = 256
HGRID = 20
WGRID = 52
STRIDE = 25

flow_shift = 5.0
norm_eps = 1e-06


def shift(value, axis, distance):
    n = lax.axis_size(axis)
    return lax.ppermute(value, axis, [(i, (i + distance) % n) for i in range(n)])


def ladder(length):
    return 10000.0 ** (-jnp.arange(length, dtype=jnp.float32) / length)


def rope_tables(tokens, token_count):
    half_dim = HEAD_DIM // 2
    side_pairs = half_dim // 3
    frame_pairs = half_dim - 2 * side_pairs
    frames = -(-token_count // (HGRID * WGRID))
    rates = jnp.repeat(
        jnp.concatenate([ladder(frame_pairs), ladder(side_pairs), ladder(side_pairs)]), 2
    )
    lane = jnp.arange(HEAD_DIM)
    sign = jnp.where(lane % 2 == 0, -1.0, 1.0).astype(jnp.float32)
    table_rows = -(-(frames + HGRID + WGRID) // 128) * 128
    entry = jnp.arange(table_rows)
    kind = jnp.where(entry < frames, 0, jnp.where(entry < frames + HGRID, 1, 2))
    place = entry - jnp.where(kind == 0, 0, jnp.where(kind == 1, frames, frames + HGRID))
    lane_kind = jnp.where(
        lane < 2 * frame_pairs, 0, jnp.where(lane < 2 * (frame_pairs + side_pairs), 1, 2)
    )
    angles = place.astype(jnp.float32)[:, None] * rates
    held = kind[:, None] == lane_kind
    table = jnp.concatenate(
        [jnp.where(held, jnp.cos(angles), 0.0), jnp.where(held, jnp.sin(angles) * sign, 0.0)],
        axis=1,
    )
    frame = tokens // (HGRID * WGRID)
    row = tokens // WGRID % HGRID + frames
    column = tokens % WGRID + (frames + HGRID)
    picked = (
        (entry == frame[..., None]) | (entry == row[..., None]) | (entry == column[..., None])
    ).astype(jnp.bfloat16)
    high = lax.reduce_precision(table, 8, 7)
    middle = lax.reduce_precision(table - high, 8, 7)
    low = lax.reduce_precision(table - high - middle, 8, 7)
    parts = jnp.concatenate([high, middle, low], axis=0).astype(jnp.bfloat16)
    return jnp.einsum(
        "...t,tl->...l",
        jnp.concatenate([picked] * 3, axis=-1),
        parts,
        preferred_element_type=jnp.float32,
    )


def stamp_embedding(step_value):
    half_freq = FREQ // 2
    inverse_rates = 10000.0 ** (-jnp.arange(half_freq, dtype=jnp.float32) / half_freq)
    phases = step_value * inverse_rates
    return jnp.concatenate([jnp.cos(phases), jnp.sin(phases)])


def noise_level(step_value):
    scaled = step_value / 1000.0
    return flow_shift * scaled / (1.0 + (flow_shift - 1.0) * scaled)


def whole():
    return pl.BlockSpec(memory_space=pltpu.VMEM)


def pack_messages(queries, keys, values, seq_index, peers):
    rows, features = queries.shape
    width = features // peers

    def kernel(index_ref, q_ref, k_ref, v_ref, *out_refs):
        base = index_ref[0]
        for d in range(peers):
            owner = lax.rem(base + d, peers)
            at = pl.multiple_of(owner * width, width)
            for part, ref in enumerate((q_ref, k_ref, v_ref)):
                out_refs[d][part * rows : (part + 1) * rows, :] = ref[:, pl.ds(at, width)]

    return pl.pallas_call(
        kernel,
        in_specs=[pl.BlockSpec(memory_space=pltpu.SMEM), whole(), whole(), whole()],
        out_specs=[whole()] * peers,
        out_shape=[jax.ShapeDtypeStruct((3 * rows, width), queries.dtype)] * peers,
        compiler_params=pltpu.CompilerParams(vmem_limit_bytes=16 * 1024 * 1024),
        name="pack_messages",
    )(seq_index.reshape(1), queries, keys, values)


def turn_rows(messages, tables, order):
    peers = len(messages)
    rows = messages[0].shape[0] // 3
    width = messages[0].shape[1]
    heads = width // HEAD_DIM
    total = peers * rows

    def kernel(*refs):
        message_refs = refs[:peers]
        table_ref, q_ref, k_ref, v_ref = refs[peers:]
        even = lax.broadcasted_iota(jnp.int32, (rows, HEAD_DIM), 1) % 2 == 0

        def one_head(h, carry):
            lanes = pl.ds(pl.multiple_of(h * HEAD_DIM, HEAD_DIM), HEAD_DIM)
            for place, d in enumerate(order):
                cos_d = table_ref[d, :, :HEAD_DIM]
                sin_d = table_ref[d, :, HEAD_DIM:]

                def turned(part):
                    x = message_refs[d][part * rows : (part + 1) * rows, lanes].astype(jnp.float32)
                    swapped = jnp.where(even, pltpu.roll(x, HEAD_DIM - 1, 1), pltpu.roll(x, 1, 1))
                    return (x * cos_d + swapped * sin_d).astype(jnp.bfloat16)

                q_ref[place * heads + h] = turned(0)
                k_ref[h, place * rows : (place + 1) * rows, :] = turned(1)
                v_ref[h, place * rows : (place + 1) * rows, :] = message_refs[d][
                    2 * rows : 3 * rows, lanes
                ]
            return carry

        lax.fori_loop(0, heads, one_head, 0)

    return pl.pallas_call(
        kernel,
        in_specs=[whole()] * (peers + 1),
        out_specs=[whole()] * 3,
        out_shape=[
            jax.ShapeDtypeStruct((peers * heads, rows, HEAD_DIM), jnp.bfloat16),
            jax.ShapeDtypeStruct((heads, total, HEAD_DIM), jnp.bfloat16),
            jax.ShapeDtypeStruct((heads, total, HEAD_DIM), jnp.bfloat16),
        ],
        compiler_params=pltpu.CompilerParams(vmem_limit_bytes=16 * 1024 * 1024),
        name="turn_rows",
    )(*messages, tables)


def attend(turned_q, turned_k, values, first, count, together):
    heads, total, _ = turned_k.shape
    rows = turned_q.shape[1]
    width = heads * HEAD_DIM
    exponent_scale = HEAD_DIM ** (-0.5) * 1.4426950408889634

    def kernel(q_ref, k_ref, v_ref, out_ref):
        def one_head(i, h):
            scores = lax.dot_general(
                q_ref[(first + i) * heads + h],
                k_ref[h],
                (((1,), (1,)), ((), ())),
                preferred_element_type=jnp.float32,
            )
            row_max = jnp.max(scores, axis=1, keepdims=True)
            weights = jnp.exp2((scores - row_max) * exponent_scale)
            row_total = jnp.sum(weights, axis=1, keepdims=True)
            mixed = lax.dot_general(
                weights.astype(jnp.bfloat16),
                v_ref[h],
                (((1,), (0,)), ((), ())),
                preferred_element_type=jnp.float32,
            )
            lanes = pl.ds(pl.multiple_of(h * HEAD_DIM, HEAD_DIM), HEAD_DIM)
            out_ref[i, :, lanes] = (mixed / row_total).astype(jnp.bfloat16)

        def one_block(step, carry):
            if together:
                for h in range(heads):
                    one_head(step, h)
            else:
                one_head(step // heads, lax.rem(step, heads))
            return carry

        lax.fori_loop(0, count if together else count * heads, one_block, 0)

    return pl.pallas_call(
        kernel,
        in_specs=[whole()] * 3,
        out_specs=whole(),
        out_shape=jax.ShapeDtypeStruct((count, rows, width), jnp.bfloat16),
        cost_estimate=pl.CostEstimate(
            flops=4 * count * rows * total * width,
            bytes_accessed=8 * total * width,
            transcendentals=heads * count * rows * total,
        ),
        compiler_params=pltpu.CompilerParams(vmem_limit_bytes=24 * 1024 * 1024),
        name="attend",
    )(turned_q, turned_k, values)


TILE = 256
STEP = 128


def message_layout(rows, columns):
    groups, rest = divmod(rows, 8)
    pieces = 8 // rest
    return groups, rest, pieces, groups * columns, (8, groups * columns + columns // pieces)


def add_partial(attention, place, weight, column_half, received):
    rows, width = attention.shape[1:]
    half = weight.shape[1] // 2
    groups, rest, pieces, body, shape = message_layout(rows, half)
    piece = half // pieces
    start = column_half * half

    def kernel(*refs):
        a_ref, w_ref = refs[:2]
        in_ref = refs[2] if received is not None else None
        out_ref = refs[-1]

        def one_tile(j, carry):
            at = pl.multiple_of(j * STEP, STEP)
            tile = jnp.dot(
                a_ref[place],
                w_ref[:, pl.ds(pl.multiple_of(start + at, STEP), STEP)],
                preferred_element_type=jnp.float32,
            )
            for t in range(groups):
                where = pl.ds(pl.multiple_of(t * half + at, STEP), STEP)
                part = tile[8 * t : 8 * t + 8, :]
                if in_ref is not None:
                    part = part + in_ref[:, where].astype(jnp.float32)
                out_ref[:, where] = part.astype(jnp.bfloat16)
            return carry

        lax.fori_loop(0, half // STEP, one_tile, 0)
        for i in range(pieces):
            part = jnp.dot(
                a_ref[place, 8 * groups : rows, :],
                w_ref[:, start + i * piece : start + (i + 1) * piece],
                preferred_element_type=jnp.float32,
            )
            if in_ref is not None:
                part = part + in_ref[i * rest : (i + 1) * rest, body:].astype(jnp.float32)
            out_ref[i * rest : (i + 1) * rest, body:] = part.astype(jnp.bfloat16)

    operands = [attention, weight] + ([] if received is None else [received])
    return pl.pallas_call(
        kernel,
        in_specs=[whole()] * len(operands),
        out_specs=whole(),
        out_shape=jax.ShapeDtypeStruct(shape, jnp.bfloat16),
        cost_estimate=pl.CostEstimate(
            flops=2 * rows * width * half, bytes_accessed=4 * rows * half, transcendentals=0
        ),
        compiler_params=pltpu.CompilerParams(vmem_limit_bytes=8 * 1024 * 1024),
        name="add_partial",
    )(*operands)


def finish_rows(attention, place, weight, messages, residual, modulation, head, latent, change):
    rows, width = attention.shape[1:]
    columns = weight.shape[1]
    half = columns // 2
    groups, rest, pieces, body, _ = message_layout(rows, half)
    piece = half // pieces
    latent_width = head.shape[0]
    tiles = half // TILE

    def kernel(
        change_ref, a_ref, w_ref, m00, m10, m01, m11, res_ref, gate_ref, shift_ref, scale_ref,
        head_ref, lat_ref,
        vel_ref, step_ref, hand_ref, hid_scr, tail_scr,
    ):
        sums = jnp.zeros((rows, TILE), jnp.float32)
        for c, pair in enumerate(((m00, m10), (m01, m11))):
            for i in range(pieces):
                tail_scr[:, i * piece : (i + 1) * piece] = pair[0][
                    i * rest : (i + 1) * rest, body:
                ].astype(jnp.float32) + pair[1][i * rest : (i + 1) * rest, body:].astype(
                    jnp.float32
                )

            def one_tile(j, sums):
                at = pl.multiple_of(j * TILE, TILE)
                column = pl.ds(pl.multiple_of(c * half + at, TILE), TILE)
                arrived = []
                for t in range(groups):
                    where = pl.ds(pl.multiple_of(t * half + at, TILE), TILE)
                    arrived.append(
                        pair[0][:, where].astype(jnp.float32)
                        + pair[1][:, where].astype(jnp.float32)
                    )
                arrived.append(tail_scr[:, pl.ds(at, TILE)])
                tile = jnp.dot(
                    a_ref[place], w_ref[:, column], preferred_element_type=jnp.float32
                ) + jnp.concatenate(arrived, axis=0)
                hidden = res_ref[:, column].astype(jnp.float32) + gate_ref[:, column] * tile
                hid_scr[:, column] = hidden
                return sums + hidden

            sums = lax.fori_loop(0, tiles, one_tile, sums)
        mean = jnp.sum(sums, axis=1, keepdims=True) / columns

        def square_tile(j, squares):
            centered = hid_scr[:, pl.ds(pl.multiple_of(j * TILE, TILE), TILE)] - mean
            return squares + centered * centered

        squares = lax.fori_loop(
            0, 2 * tiles, square_tile, jnp.zeros((rows, TILE), jnp.float32)
        )
        variance = jnp.sum(squares, axis=1, keepdims=True) / columns
        inverse = lax.rsqrt(variance + norm_eps)

        def head_tile(j, velocity):
            column = pl.ds(pl.multiple_of(j * TILE, TILE), TILE)
            normed = (hid_scr[:, column] - mean) * inverse * (
                1.0 + scale_ref[:, column]
            ) + shift_ref[:, column]
            return velocity + lax.dot_general(
                head_ref[:, column],
                normed.astype(jnp.bfloat16),
                (((1,), (1,)), ((), ())),
                preferred_element_type=jnp.float32,
            )

        velocity = lax.fori_loop(
            0, 2 * tiles, head_tile, jnp.zeros((latent_width, rows), jnp.float32)
        )
        vel_ref[...] = velocity
        stepped = lat_ref[...] + change_ref[0] * velocity
        step_ref[...] = stepped
        hand_ref[...] = stepped.astype(jnp.bfloat16)

    small = jax.ShapeDtypeStruct((latent_width, rows), jnp.float32)
    return pl.pallas_call(
        kernel,
        in_specs=[pl.BlockSpec(memory_space=pltpu.SMEM)] + [whole()] * 12,
        out_specs=[whole()] * 3,
        out_shape=[small, small, jax.ShapeDtypeStruct(small.shape, jnp.bfloat16)],
        scratch_shapes=[
            pltpu.VMEM((rows, columns), jnp.float32),
            pltpu.VMEM((rest, half), jnp.float32),
        ],
        compiler_params=pltpu.CompilerParams(vmem_limit_bytes=16 * 1024 * 1024),
        name="finish_rows",
    )(change.reshape(1), attention, weight, *messages, residual, *modulation, head, latent)


def join_latents(rows, first_order, own_tokens, stepped, velocity, change, is_low):
    peers, latent_width, block_rows = rows.shape

    def kernel(change_ref, low_ref, rows_ref, order_ref, own_ref, step_ref, vel_ref, out_ref):
        own = own_ref[...]
        started = jnp.zeros((latent_width, block_rows), jnp.float32)
        for d in range(peers):
            same = (own == order_ref[d : d + 1, :]).astype(jnp.float32).astype(jnp.bfloat16)
            started += lax.dot_general(
                rows_ref[d], same, (((1,), (1,)), ((), ())), preferred_element_type=jnp.float32
            )
        finished = started + change_ref[0] * vel_ref[...]
        out_ref[...] = jnp.where(low_ref[0] == 1, finished, step_ref[...])

    scalar = pl.BlockSpec(memory_space=pltpu.SMEM)
    return pl.pallas_call(
        kernel,
        in_specs=[scalar, scalar] + [whole()] * 5,
        out_specs=whole(),
        out_shape=jax.ShapeDtypeStruct((latent_width, block_rows), jnp.float32),
        compiler_params=pltpu.CompilerParams(vmem_limit_bytes=16 * 1024 * 1024),
        name="join_latents",
    )(change.reshape(1), is_low.reshape(1), rows, first_order, own_tokens, stepped, velocity)


def shards(
    query_heads,
    key_heads,
    value_heads,
    residual,
    out_weight,
    mod_weight,
    head_weight,
    latent,
    timesteps,
    token_order,
):
    peers = lax.axis_size("seq")
    seq_index = lax.axis_index("seq")
    expert_index = lax.axis_index("expert")
    block_rows = query_heads.shape[2]
    model_width = residual.shape[3]
    far = peers // 2

    outgoing = pack_messages(
        query_heads[0, 0], key_heads[0, 0], value_heads[0, 0], seq_index, peers
    )
    arrived = [None] * peers
    arrived[0] = outgoing[0]
    order = [far]
    for d in range(far - 1, 0, -1):
        order += [d, peers - d]
    for d in order:
        arrived[d] = shift(outgoing[d], "seq", d)
    order.append(0)

    orders = lax.dynamic_index_in_dim(token_order, expert_index, 0, keepdims=False)[0]
    by_device = orders.reshape(peers, block_rows)
    doubled = jnp.concatenate([by_device[::-1], by_device[::-1]], axis=0)
    slot_tokens = lax.dynamic_slice_in_dim(doubled, peers - 1 - seq_index, peers, axis=0)
    own_tokens = slot_tokens[0]
    tables = rope_tables(slot_tokens, token_order.shape[2])

    step_value = timesteps[0, 0].astype(jnp.float32)
    embedded = stamp_embedding(step_value).astype(jnp.bfloat16)
    modulation = jnp.dot(embedded[None], mod_weight[0], preferred_element_type=jnp.float32)
    modulation = [
        modulation[:, i * model_width : (i + 1) * model_width] for i in range(3)
    ]
    change = noise_level(step_value - STRIDE) - noise_level(step_value)

    first_order = token_order[0, 0].reshape(peers, block_rows)
    tables, modulation, change, first_order, own_column = lax.optimization_barrier(
        (tables, modulation, change, first_order, own_tokens[:, None])
    )

    turned_q, turned_k, values = turn_rows(arrived, tables, order)
    attended = {}
    first = 0
    for count in (3, 6, peers - 9):
        block = attend(turned_q, turned_k, values, first, count, first == 0)
        for i in range(count):
            attended[order[first + i]] = (block, i)
        first += count

    weight = out_weight[0]
    chains = {(way, c): None for way in (1, -1) for c in (0, 1)}
    for way, c in ((1, 0), (-1, 1)):
        chains[way, c] = shift(add_partial(*attended[far], weight, c, None), "seq", way)
    for distance in range(far - 1, 0, -1):
        for way, c in ((1, 1), (-1, 0), (1, 0), (-1, 1)):
            source = attended[-way * distance % peers]
            chains[way, c] = shift(add_partial(*source, weight, c, chains[way, c]), "seq", way)
    velocity, stepped, handed = finish_rows(
        *attended[0],
        weight,
        [chains[1, 0], chains[-1, 0], chains[1, 1], chains[-1, 1]],
        residual[0, 0],
        modulation,
        head_weight[0].T,
        latent[0].T,
        change,
    )

    handed = lax.ppermute(handed, "expert", [(0, 1)])
    rows = lax.all_gather(handed, "seq", axis=0)
    finished = join_latents(
        rows, first_order, own_column, stepped, velocity, change, expert_index
    )
    return (velocity.T[None, None], finished.T[None, None])


def solution(mesh):
    return jax.shard_map(
        shards,
        mesh=mesh,
        in_specs=(
            P("expert", "groups", "seq", None),
            P("expert", "groups", "seq", None),
            P("expert", "groups", "seq", None),
            P("expert", "groups", "seq", None),
            P("expert", "seq", None),
            P("expert", None, None),
            P("expert", None, None),
            P("groups", "seq", None),
            P("expert", "groups"),
            P(None, "groups", None),
        ),
        out_specs=(P("expert", "groups", "seq", None), P("expert", "groups", "seq", None)),
        check_vma=False,
    )
```

```python
import jax
import jax.numpy as jnp
from jax import lax
from jax.experimental import pallas as pl
from jax.experimental.pallas import tpu as pltpu
from jax.sharding import PartitionSpec as P

HEAD_DIM = 128
FREQ = 256
HGRID = 20
WGRID = 52
STRIDE = 25

flow_shift = 5.0
norm_eps = 1e-06


def shift(value, axis, distance):
    n = lax.axis_size(axis)
    return lax.ppermute(value, axis, [(i, (i + distance) % n) for i in range(n)])


def ladder(length):
    return 10000.0 ** (-jnp.arange(length, dtype=jnp.float32) / length)


def rope_tables(tokens, token_count):
    half_dim = HEAD_DIM // 2
    side_pairs = half_dim // 3
    frame_pairs = half_dim - 2 * side_pairs
    frames = -(-token_count // (HGRID * WGRID))
    rates = jnp.repeat(
        jnp.concatenate([ladder(frame_pairs), ladder(side_pairs), ladder(side_pairs)]), 2
    )
    lane = jnp.arange(HEAD_DIM)
    sign = jnp.where(lane % 2 == 0, -1.0, 1.0).astype(jnp.float32)
    table_rows = -(-(frames + HGRID + WGRID) // 128) * 128
    entry = jnp.arange(table_rows)
    kind = jnp.where(entry < frames, 0, jnp.where(entry < frames + HGRID, 1, 2))
    place = entry - jnp.where(kind == 0, 0, jnp.where(kind == 1, frames, frames + HGRID))
    lane_kind = jnp.where(
        lane < 2 * frame_pairs, 0, jnp.where(lane < 2 * (frame_pairs + side_pairs), 1, 2)
    )
    angles = place.astype(jnp.float32)[:, None] * rates
    held = kind[:, None] == lane_kind
    table = jnp.concatenate(
        [jnp.where(held, jnp.cos(angles), 0.0), jnp.where(held, jnp.sin(angles) * sign, 0.0)],
        axis=1,
    )
    frame = tokens // (HGRID * WGRID)
    row = tokens // WGRID % HGRID + frames
    column = tokens % WGRID + (frames + HGRID)
    picked = (
        (entry == frame[..., None]) | (entry == row[..., None]) | (entry == column[..., None])
    ).astype(jnp.bfloat16)
    high = lax.reduce_precision(table, 8, 7)
    middle = lax.reduce_precision(table - high, 8, 7)
    low = lax.reduce_precision(table - high - middle, 8, 7)
    parts = jnp.concatenate([high, middle, low], axis=0).astype(jnp.bfloat16)
    return jnp.einsum(
        "...t,tl->...l",
        jnp.concatenate([picked] * 3, axis=-1),
        parts,
        preferred_element_type=jnp.float32,
    )


def stamp_embedding(step_value):
    half_freq = FREQ // 2
    inverse_rates = 10000.0 ** (-jnp.arange(half_freq, dtype=jnp.float32) / half_freq)
    phases = step_value * inverse_rates
    return jnp.concatenate([jnp.cos(phases), jnp.sin(phases)])


def noise_level(step_value):
    scaled = step_value / 1000.0
    return flow_shift * scaled / (1.0 + (flow_shift - 1.0) * scaled)


def whole():
    return pl.BlockSpec(memory_space=pltpu.VMEM)


def pack_messages(queries, keys, values, seq_index, is_low, peers):
    rows, features = queries.shape
    width = features // peers

    def kernel(index_ref, low_ref, q_ref, k_ref, v_ref, *out_refs):
        base = index_ref[0]

        @pl.when(low_ref[0] == 1)
        def _():
            pl.delay(LAG_NANOSECONDS)

        for d in range(peers):
            owner = lax.rem(base + d, peers)
            at = pl.multiple_of(owner * width, width)
            for part, ref in enumerate((q_ref, k_ref, v_ref)):
                out_refs[d][part * rows : (part + 1) * rows, :] = ref[:, pl.ds(at, width)]

    return pl.pallas_call(
        kernel,
        in_specs=[pl.BlockSpec(memory_space=pltpu.SMEM)] * 2 + [whole()] * 3,
        out_specs=[whole()] * peers,
        out_shape=[jax.ShapeDtypeStruct((3 * rows, width), queries.dtype)] * peers,
        compiler_params=pltpu.CompilerParams(vmem_limit_bytes=16 * 1024 * 1024),
        name="pack_messages",
    )(seq_index.reshape(1), is_low.reshape(1), queries, keys, values)


def turn_rows(messages, tables, order):
    peers = len(messages)
    rows = messages[0].shape[0] // 3
    width = messages[0].shape[1]
    heads = width // HEAD_DIM
    total = peers * rows

    def kernel(*refs):
        message_refs = refs[:peers]
        table_ref, q_ref, k_ref, v_ref = refs[peers:]
        even = lax.broadcasted_iota(jnp.int32, (rows, HEAD_DIM), 1) % 2 == 0

        def one_head(h, carry):
            lanes = pl.ds(pl.multiple_of(h * HEAD_DIM, HEAD_DIM), HEAD_DIM)
            for place, d in enumerate(order):
                cos_d = table_ref[d, :, :HEAD_DIM]
                sin_d = table_ref[d, :, HEAD_DIM:]

                def turned(part):
                    x = message_refs[d][part * rows : (part + 1) * rows, lanes].astype(jnp.float32)
                    swapped = jnp.where(even, pltpu.roll(x, HEAD_DIM - 1, 1), pltpu.roll(x, 1, 1))
                    return (x * cos_d + swapped * sin_d).astype(jnp.bfloat16)

                q_ref[place * heads + h] = turned(0)
                k_ref[h, place * rows : (place + 1) * rows, :] = turned(1)
                v_ref[h, place * rows : (place + 1) * rows, :] = message_refs[d][
                    2 * rows : 3 * rows, lanes
                ]
            return carry

        lax.fori_loop(0, heads, one_head, 0)

    return pl.pallas_call(
        kernel,
        in_specs=[whole()] * (peers + 1),
        out_specs=[whole()] * 3,
        out_shape=[
            jax.ShapeDtypeStruct((peers * heads, rows, HEAD_DIM), jnp.bfloat16),
            jax.ShapeDtypeStruct((heads, total, HEAD_DIM), jnp.bfloat16),
            jax.ShapeDtypeStruct((heads, total, HEAD_DIM), jnp.bfloat16),
        ],
        compiler_params=pltpu.CompilerParams(vmem_limit_bytes=16 * 1024 * 1024),
        name="turn_rows",
    )(*messages, tables)


def attend(turned_q, turned_k, values, first, count, together):
    heads, total, _ = turned_k.shape
    rows = turned_q.shape[1]
    width = heads * HEAD_DIM
    exponent_scale = HEAD_DIM ** (-0.5) * 1.4426950408889634

    def kernel(q_ref, k_ref, v_ref, out_ref):
        def one_head(i, h):
            scores = lax.dot_general(
                q_ref[(first + i) * heads + h],
                k_ref[h],
                (((1,), (1,)), ((), ())),
                preferred_element_type=jnp.float32,
            )
            row_max = jnp.max(scores, axis=1, keepdims=True)
            weights = jnp.exp2((scores - row_max) * exponent_scale)
            row_total = jnp.sum(weights, axis=1, keepdims=True)
            mixed = lax.dot_general(
                weights.astype(jnp.bfloat16),
                v_ref[h],
                (((1,), (0,)), ((), ())),
                preferred_element_type=jnp.float32,
            )
            lanes = pl.ds(pl.multiple_of(h * HEAD_DIM, HEAD_DIM), HEAD_DIM)
            out_ref[i, :, lanes] = (mixed / row_total).astype(jnp.bfloat16)

        def one_block(step, carry):
            if together:
                for h in range(heads):
                    one_head(step, h)
            else:
                one_head(step // heads, lax.rem(step, heads))
            return carry

        lax.fori_loop(0, count if together else count * heads, one_block, 0)

    return pl.pallas_call(
        kernel,
        in_specs=[whole()] * 3,
        out_specs=whole(),
        out_shape=jax.ShapeDtypeStruct((count, rows, width), jnp.bfloat16),
        cost_estimate=pl.CostEstimate(
            flops=4 * count * rows * total * width,
            bytes_accessed=8 * total * width,
            transcendentals=heads * count * rows * total,
        ),
        compiler_params=pltpu.CompilerParams(vmem_limit_bytes=24 * 1024 * 1024),
        name="attend",
    )(turned_q, turned_k, values)


TILE = 256
LAG_NANOSECONDS = 42000


def message_layout(rows, columns):
    groups, rest = divmod(rows, 8)
    pieces = 8 // rest
    return groups, rest, pieces, groups * columns, (8, groups * columns + columns // pieces)


def add_partial(attention, place, weight, column_half, received, step):
    rows, width = attention.shape[1:]
    half = weight.shape[1] // 2
    groups, rest, pieces, body, shape = message_layout(rows, half)
    piece = half // pieces
    start = column_half * half

    def kernel(*refs):
        a_ref, w_ref = refs[:2]
        in_ref = refs[2] if received is not None else None
        out_ref = refs[-1]

        def one_tile(j, carry):
            at = pl.multiple_of(j * step, step)
            tile = jnp.dot(
                a_ref[place],
                w_ref[:, pl.ds(pl.multiple_of(start + at, step), step)],
                preferred_element_type=jnp.float32,
            )
            for t in range(groups):
                where = pl.ds(pl.multiple_of(t * half + at, step), step)
                part = tile[8 * t : 8 * t + 8, :]
                if in_ref is not None:
                    part = part + in_ref[:, where].astype(jnp.float32)
                out_ref[:, where] = part.astype(jnp.bfloat16)
            return carry

        lax.fori_loop(0, half // step, one_tile, 0)
        for i in range(pieces):
            part = jnp.dot(
                a_ref[place, 8 * groups : rows, :],
                w_ref[:, start + i * piece : start + (i + 1) * piece],
                preferred_element_type=jnp.float32,
            )
            if in_ref is not None:
                part = part + in_ref[i * rest : (i + 1) * rest, body:].astype(jnp.float32)
            out_ref[i * rest : (i + 1) * rest, body:] = part.astype(jnp.bfloat16)

    operands = [attention, weight] + ([] if received is None else [received])
    return pl.pallas_call(
        kernel,
        in_specs=[whole()] * len(operands),
        out_specs=whole(),
        out_shape=jax.ShapeDtypeStruct(shape, jnp.bfloat16),
        cost_estimate=pl.CostEstimate(
            flops=2 * rows * width * half, bytes_accessed=4 * rows * half, transcendentals=0
        ),
        compiler_params=pltpu.CompilerParams(vmem_limit_bytes=8 * 1024 * 1024),
        name="add_partial",
    )(*operands)


def finish_rows(attention, place, weight, messages, residual, modulation, head, latent, change):
    rows, width = attention.shape[1:]
    columns = weight.shape[1]
    half = columns // 2
    groups, rest, pieces, body, _ = message_layout(rows, half)
    piece = half // pieces
    latent_width = head.shape[0]
    tiles = half // TILE

    def kernel(
        change_ref, a_ref, w_ref, m00, m10, m01, m11, res_ref, gate_ref, shift_ref, scale_ref,
        head_ref, lat_ref,
        vel_ref, step_ref, hand_ref, hid_scr, tail_scr,
    ):
        sums = jnp.zeros((rows, TILE), jnp.float32)
        for c, pair in enumerate(((m00, m10), (m01, m11))):
            for i in range(pieces):
                tail_scr[:, i * piece : (i + 1) * piece] = pair[0][
                    i * rest : (i + 1) * rest, body:
                ].astype(jnp.float32) + pair[1][i * rest : (i + 1) * rest, body:].astype(
                    jnp.float32
                )

            def one_tile(j, sums):
                at = pl.multiple_of(j * TILE, TILE)
                column = pl.ds(pl.multiple_of(c * half + at, TILE), TILE)
                arrived = []
                for t in range(groups):
                    where = pl.ds(pl.multiple_of(t * half + at, TILE), TILE)
                    arrived.append(
                        pair[0][:, where].astype(jnp.float32)
                        + pair[1][:, where].astype(jnp.float32)
                    )
                arrived.append(tail_scr[:, pl.ds(at, TILE)])
                tile = jnp.dot(
                    a_ref[place], w_ref[:, column], preferred_element_type=jnp.float32
                ) + jnp.concatenate(arrived, axis=0)
                hidden = res_ref[:, column].astype(jnp.float32) + gate_ref[:, column] * tile
                hid_scr[:, column] = hidden
                return sums + hidden

            sums = lax.fori_loop(0, tiles, one_tile, sums)
        mean = jnp.sum(sums, axis=1, keepdims=True) / columns

        def square_tile(j, squares):
            centered = hid_scr[:, pl.ds(pl.multiple_of(j * TILE, TILE), TILE)] - mean
            return squares + centered * centered

        squares = lax.fori_loop(
            0, 2 * tiles, square_tile, jnp.zeros((rows, TILE), jnp.float32)
        )
        variance = jnp.sum(squares, axis=1, keepdims=True) / columns
        inverse = lax.rsqrt(variance + norm_eps)

        def head_tile(j, velocity):
            column = pl.ds(pl.multiple_of(j * TILE, TILE), TILE)
            normed = (hid_scr[:, column] - mean) * inverse * (
                1.0 + scale_ref[:, column]
            ) + shift_ref[:, column]
            return velocity + lax.dot_general(
                head_ref[:, column],
                normed.astype(jnp.bfloat16),
                (((1,), (1,)), ((), ())),
                preferred_element_type=jnp.float32,
            )

        velocity = lax.fori_loop(
            0, 2 * tiles, head_tile, jnp.zeros((latent_width, rows), jnp.float32)
        )
        vel_ref[...] = velocity
        stepped = lat_ref[...] + change_ref[0] * velocity
        step_ref[...] = stepped
        hand_ref[...] = stepped.astype(jnp.bfloat16)

    small = jax.ShapeDtypeStruct((latent_width, rows), jnp.float32)
    return pl.pallas_call(
        kernel,
        in_specs=[pl.BlockSpec(memory_space=pltpu.SMEM)] + [whole()] * 12,
        out_specs=[whole()] * 3,
        out_shape=[small, small, jax.ShapeDtypeStruct(small.shape, jnp.bfloat16)],
        scratch_shapes=[
            pltpu.VMEM((rows, columns), jnp.float32),
            pltpu.VMEM((rest, half), jnp.float32),
        ],
        compiler_params=pltpu.CompilerParams(vmem_limit_bytes=16 * 1024 * 1024),
        name="finish_rows",
    )(change.reshape(1), attention, weight, *messages, residual, *modulation, head, latent)


def join_latents(rows, first_order, own_tokens, stepped, velocity, change, is_low):
    peers, latent_width, block_rows = rows.shape

    def kernel(change_ref, low_ref, rows_ref, order_ref, own_ref, step_ref, vel_ref, out_ref):
        own = own_ref[...]
        started = jnp.zeros((latent_width, block_rows), jnp.float32)
        for d in range(peers):
            same = (own == order_ref[d : d + 1, :]).astype(jnp.float32).astype(jnp.bfloat16)
            started += lax.dot_general(
                rows_ref[d], same, (((1,), (1,)), ((), ())), preferred_element_type=jnp.float32
            )
        finished = started + change_ref[0] * vel_ref[...]
        out_ref[...] = jnp.where(low_ref[0] == 1, finished, step_ref[...])

    scalar = pl.BlockSpec(memory_space=pltpu.SMEM)
    return pl.pallas_call(
        kernel,
        in_specs=[scalar, scalar] + [whole()] * 5,
        out_specs=whole(),
        out_shape=jax.ShapeDtypeStruct((latent_width, block_rows), jnp.float32),
        compiler_params=pltpu.CompilerParams(vmem_limit_bytes=16 * 1024 * 1024),
        name="join_latents",
    )(change.reshape(1), is_low.reshape(1), rows, first_order, own_tokens, stepped, velocity)


def shards(
    query_heads,
    key_heads,
    value_heads,
    residual,
    out_weight,
    mod_weight,
    head_weight,
    latent,
    timesteps,
    token_order,
):
    peers = lax.axis_size("seq")
    seq_index = lax.axis_index("seq")
    expert_index = lax.axis_index("expert")
    block_rows = query_heads.shape[2]
    model_width = residual.shape[3]
    far = peers // 2

    outgoing = pack_messages(
        query_heads[0, 0], key_heads[0, 0], value_heads[0, 0], seq_index, expert_index, peers
    )
    arrived = [None] * peers
    arrived[0] = outgoing[0]
    order = [far]
    for d in range(far - 1, 0, -1):
        order += [d, peers - d]
    for d in order:
        arrived[d] = shift(outgoing[d], "seq", d)
    order.append(0)

    orders = lax.dynamic_index_in_dim(token_order, expert_index, 0, keepdims=False)[0]
    by_device = orders.reshape(peers, block_rows)
    doubled = jnp.concatenate([by_device[::-1], by_device[::-1]], axis=0)
    slot_tokens = lax.dynamic_slice_in_dim(doubled, peers - 1 - seq_index, peers, axis=0)
    own_tokens = slot_tokens[0]
    tables = rope_tables(slot_tokens, token_order.shape[2])

    step_value = timesteps[0, 0].astype(jnp.float32)
    embedded = stamp_embedding(step_value).astype(jnp.bfloat16)
    modulation = jnp.dot(embedded[None], mod_weight[0], preferred_element_type=jnp.float32)
    modulation = [
        modulation[:, i * model_width : (i + 1) * model_width] for i in range(3)
    ]
    change = noise_level(step_value - STRIDE) - noise_level(step_value)

    first_order = jnp.take(
        token_order[0, 0].reshape(peers, block_rows),
        seq_index ^ jnp.arange(peers),
        axis=0,
        mode="clip",
    )
    tables, modulation, change, first_order, own_column = lax.optimization_barrier(
        (tables, modulation, change, first_order, own_tokens[:, None])
    )

    turned_q, turned_k, values = turn_rows(arrived, tables, order)
    attended = {}
    first = 0
    for count in (3, 6, peers - 9):
        block = attend(turned_q, turned_k, values, first, count, False)
        for i in range(count):
            attended[order[first + i]] = (block, i)
        first += count

    weight = out_weight[0]
    chains = {(way, c): None for way in (1, -1) for c in (0, 1)}
    for way, c in ((1, 0), (-1, 1)):
        chains[way, c] = shift(
            add_partial(*attended[far], weight, c, None, 256), "seq", way
        )
    for distance in range(far - 1, 0, -1):
        for way, c in ((1, 1), (-1, 0), (1, 0), (-1, 1)):
            source = attended[-way * distance % peers]
            step = 512 if distance <= 3 else 256
            chains[way, c] = shift(
                add_partial(*source, weight, c, chains[way, c], step), "seq", way
            )
    velocity, stepped, handed = finish_rows(
        *attended[0],
        weight,
        [chains[1, 0], chains[-1, 0], chains[1, 1], chains[-1, 1]],
        residual[0, 0],
        modulation,
        head_weight[0].T,
        latent[0].T,
        change,
    )

    rows = handed[None]
    for bit in range(peers.bit_length() - 1):
        pairs = [(i, i ^ 1 << bit) for i in range(peers)]
        rows = jnp.concatenate([rows, lax.ppermute(rows, ("expert", "seq"), pairs)], axis=0)
    rows = lax.ppermute(rows, "expert", [(0, 1)])
    finished = join_latents(
        rows, first_order, own_column, stepped, velocity, change, expert_index
    )
    return (velocity.T[None, None], finished.T[None, None])


def solution(mesh):
    return jax.shard_map(
        shards,
        mesh=mesh,
        in_specs=(
            P("expert", "groups", "seq", None),
            P("expert", "groups", "seq", None),
            P("expert", "groups", "seq", None),
            P("expert", "groups", "seq", None),
            P("expert", "seq", None),
            P("expert", None, None),
            P("expert", None, None),
            P("groups", "seq", None),
            P("expert", "groups"),
            P(None, "groups", None),
        ),
        out_specs=(P("expert", "groups", "seq", None), P("expert", "groups", "seq", None)),
        check_vma=False,
    )
```

```python
import jax
import jax.numpy as jnp
from jax import lax
from jax.experimental import pallas as pl
from jax.experimental.pallas import tpu as pltpu
from jax.sharding import PartitionSpec as P

HEAD_DIM = 128
FREQ = 256
HGRID = 20
WGRID = 52
STRIDE = 25

flow_shift = 5.0
norm_eps = 1e-06


def shift(value, axis, distance):
    n = lax.axis_size(axis)
    return lax.ppermute(value, axis, [(i, (i + distance) % n) for i in range(n)])


def ladder(length):
    return 10000.0 ** (-jnp.arange(length, dtype=jnp.float32) / length)


def rope_tables(tokens, token_count):
    half_dim = HEAD_DIM // 2
    side_pairs = half_dim // 3
    frame_pairs = half_dim - 2 * side_pairs
    frames = -(-token_count // (HGRID * WGRID))
    rates = jnp.repeat(
        jnp.concatenate([ladder(frame_pairs), ladder(side_pairs), ladder(side_pairs)]), 2
    )
    lane = jnp.arange(HEAD_DIM)
    sign = jnp.where(lane % 2 == 0, -1.0, 1.0).astype(jnp.float32)
    table_rows = -(-(frames + HGRID + WGRID) // 128) * 128
    entry = jnp.arange(table_rows)
    kind = jnp.where(entry < frames, 0, jnp.where(entry < frames + HGRID, 1, 2))
    place = entry - jnp.where(kind == 0, 0, jnp.where(kind == 1, frames, frames + HGRID))
    lane_kind = jnp.where(
        lane < 2 * frame_pairs, 0, jnp.where(lane < 2 * (frame_pairs + side_pairs), 1, 2)
    )
    angles = place.astype(jnp.float32)[:, None] * rates
    held = kind[:, None] == lane_kind
    table = jnp.concatenate(
        [jnp.where(held, jnp.cos(angles), 0.0), jnp.where(held, jnp.sin(angles) * sign, 0.0)],
        axis=1,
    )
    frame = tokens // (HGRID * WGRID)
    row = tokens // WGRID % HGRID + frames
    column = tokens % WGRID + (frames + HGRID)
    picked = (
        (entry == frame[..., None]) | (entry == row[..., None]) | (entry == column[..., None])
    ).astype(jnp.bfloat16)
    high = lax.reduce_precision(table, 8, 7)
    middle = lax.reduce_precision(table - high, 8, 7)
    low = lax.reduce_precision(table - high - middle, 8, 7)
    parts = jnp.concatenate([high, middle, low], axis=0).astype(jnp.bfloat16)
    return jnp.einsum(
        "...t,tl->...l",
        jnp.concatenate([picked] * 3, axis=-1),
        parts,
        preferred_element_type=jnp.float32,
    )


def stamp_embedding(step_value):
    half_freq = FREQ // 2
    inverse_rates = 10000.0 ** (-jnp.arange(half_freq, dtype=jnp.float32) / half_freq)
    phases = step_value * inverse_rates
    return jnp.concatenate([jnp.cos(phases), jnp.sin(phases)])


def noise_level(step_value):
    scaled = step_value / 1000.0
    return flow_shift * scaled / (1.0 + (flow_shift - 1.0) * scaled)


def whole():
    return pl.BlockSpec(memory_space=pltpu.VMEM)


def pack_messages(queries, keys, values, seq_index, is_low, peers):
    rows, features = queries.shape
    width = features // peers

    def kernel(index_ref, low_ref, q_ref, k_ref, v_ref, *out_refs):
        base = index_ref[0]

        @pl.when(low_ref[0] == 1)
        def _():
            pl.delay(LAG_NANOSECONDS)

        for d in range(peers):
            owner = lax.rem(base + d, peers)
            at = pl.multiple_of(owner * width, width)
            for part, ref in enumerate((q_ref, k_ref, v_ref)):
                out_refs[d][part * rows : (part + 1) * rows, :] = ref[:, pl.ds(at, width)]

    return pl.pallas_call(
        kernel,
        in_specs=[pl.BlockSpec(memory_space=pltpu.SMEM)] * 2 + [whole()] * 3,
        out_specs=[whole()] * peers,
        out_shape=[jax.ShapeDtypeStruct((3 * rows, width), queries.dtype)] * peers,
        compiler_params=pltpu.CompilerParams(vmem_limit_bytes=16 * 1024 * 1024),
        name="pack_messages",
    )(seq_index.reshape(1), is_low.reshape(1), queries, keys, values)


def turn_rows(messages, tables, order):
    peers = len(messages)
    rows = messages[0].shape[0] // 3
    width = messages[0].shape[1]
    heads = width // HEAD_DIM
    total = peers * rows

    def kernel(*refs):
        message_refs = refs[:peers]
        table_ref, q_ref, k_ref, v_ref = refs[peers:]
        even = lax.broadcasted_iota(jnp.int32, (rows, HEAD_DIM), 1) % 2 == 0

        def one_head(h, carry):
            lanes = pl.ds(pl.multiple_of(h * HEAD_DIM, HEAD_DIM), HEAD_DIM)
            for place, d in enumerate(order):
                cos_d = table_ref[d, :, :HEAD_DIM]
                sin_d = table_ref[d, :, HEAD_DIM:]

                def turned(part):
                    x = message_refs[d][part * rows : (part + 1) * rows, lanes].astype(jnp.float32)
                    swapped = jnp.where(even, pltpu.roll(x, HEAD_DIM - 1, 1), pltpu.roll(x, 1, 1))
                    return (x * cos_d + swapped * sin_d).astype(jnp.bfloat16)

                q_ref[place * heads + h] = turned(0)
                k_ref[h, place * rows : (place + 1) * rows, :] = turned(1)
                v_ref[h, place * rows : (place + 1) * rows, :] = message_refs[d][
                    2 * rows : 3 * rows, lanes
                ]
            return carry

        lax.fori_loop(0, heads, one_head, 0)

    return pl.pallas_call(
        kernel,
        in_specs=[whole()] * (peers + 1),
        out_specs=[whole()] * 3,
        out_shape=[
            jax.ShapeDtypeStruct((peers * heads, rows, HEAD_DIM), jnp.bfloat16),
            jax.ShapeDtypeStruct((heads, total, HEAD_DIM), jnp.bfloat16),
            jax.ShapeDtypeStruct((heads, total, HEAD_DIM), jnp.bfloat16),
        ],
        compiler_params=pltpu.CompilerParams(vmem_limit_bytes=16 * 1024 * 1024),
        name="turn_rows",
    )(*messages, tables)


def attend(turned_q, turned_k, values, first, count, together):
    heads, total, _ = turned_k.shape
    rows = turned_q.shape[1]
    width = heads * HEAD_DIM
    exponent_scale = HEAD_DIM ** (-0.5) * 1.4426950408889634

    def kernel(q_ref, k_ref, v_ref, out_ref):
        def one_head(i, h):
            scores = lax.dot_general(
                q_ref[(first + i) * heads + h],
                k_ref[h],
                (((1,), (1,)), ((), ())),
                preferred_element_type=jnp.float32,
            )
            row_max = jnp.max(scores, axis=1, keepdims=True)
            weights = jnp.exp2((scores - row_max) * exponent_scale)
            row_total = jnp.sum(weights, axis=1, keepdims=True)
            mixed = lax.dot_general(
                weights.astype(jnp.bfloat16),
                v_ref[h],
                (((1,), (0,)), ((), ())),
                preferred_element_type=jnp.float32,
            )
            lanes = pl.ds(pl.multiple_of(h * HEAD_DIM, HEAD_DIM), HEAD_DIM)
            out_ref[i, :, lanes] = (mixed / row_total).astype(jnp.bfloat16)

        def one_block(step, carry):
            if together:
                for h in range(heads):
                    one_head(step, h)
            else:
                one_head(step // heads, lax.rem(step, heads))
            return carry

        lax.fori_loop(0, count if together else count * heads, one_block, 0)

    return pl.pallas_call(
        kernel,
        in_specs=[whole()] * 3,
        out_specs=whole(),
        out_shape=jax.ShapeDtypeStruct((count, rows, width), jnp.bfloat16),
        cost_estimate=pl.CostEstimate(
            flops=4 * count * rows * total * width,
            bytes_accessed=8 * total * width,
            transcendentals=heads * count * rows * total,
        ),
        compiler_params=pltpu.CompilerParams(vmem_limit_bytes=24 * 1024 * 1024),
        name="attend",
    )(turned_q, turned_k, values)


TILE = 512
LAG_NANOSECONDS = 58000


def message_layout(rows, columns):
    groups, rest = divmod(rows, 8)
    pieces = 8 // rest
    return groups, rest, pieces, groups * columns, (8, groups * columns + columns // pieces)


def add_partial(attention, place, weight, column_half, received, step):
    rows, width = attention.shape[1:]
    half = weight.shape[1] // 2
    groups, rest, pieces, body, shape = message_layout(rows, half)
    piece = half // pieces
    start = column_half * half

    def kernel(*refs):
        a_ref, w_ref = refs[:2]
        in_ref = refs[2] if received is not None else None
        out_ref, rest_scr = refs[-2:]

        def one_tile(j, carry):
            at = pl.multiple_of(j * step, step)
            tile = jnp.dot(
                a_ref[place],
                w_ref[:, pl.ds(pl.multiple_of(start + at, step), step)],
                preferred_element_type=jnp.float32,
            )
            for t in range(groups):
                where = pl.ds(pl.multiple_of(t * half + at, step), step)
                part = tile[8 * t : 8 * t + 8, :]
                if in_ref is not None:
                    part = part + in_ref[:, where].astype(jnp.float32)
                out_ref[:, where] = part.astype(jnp.bfloat16)
            rest_scr[:, pl.ds(at, step)] = tile[8 * groups :, :]
            return carry

        lax.fori_loop(0, half // step, one_tile, 0)
        for i in range(pieces):
            part = rest_scr[:, i * piece : (i + 1) * piece]
            if in_ref is not None:
                part = part + in_ref[i * rest : (i + 1) * rest, body:].astype(jnp.float32)
            out_ref[i * rest : (i + 1) * rest, body:] = part.astype(jnp.bfloat16)

    operands = [attention, weight] + ([] if received is None else [received])
    return pl.pallas_call(
        kernel,
        in_specs=[whole()] * len(operands),
        out_specs=whole(),
        out_shape=jax.ShapeDtypeStruct(shape, jnp.bfloat16),
        scratch_shapes=[pltpu.VMEM((rest, half), jnp.float32)],
        cost_estimate=pl.CostEstimate(
            flops=2 * rows * width * half, bytes_accessed=4 * rows * half, transcendentals=0
        ),
        compiler_params=pltpu.CompilerParams(vmem_limit_bytes=8 * 1024 * 1024),
        name="add_partial",
    )(*operands)


def finish_rows(attention, place, weight, messages, residual, modulation, head, latent, change):
    rows, width = attention.shape[1:]
    columns = weight.shape[1]
    half = columns // 2
    groups, rest, pieces, body, _ = message_layout(rows, half)
    piece = half // pieces
    latent_width = head.shape[0]
    tiles = half // TILE

    def kernel(
        change_ref, a_ref, w_ref, m00, m10, m01, m11, res_ref, gate_ref, shift_ref, scale_ref,
        head_ref, lat_ref,
        vel_ref, step_ref, hand_ref, hid_scr, tail_scr,
    ):
        sums = jnp.zeros((rows, TILE), jnp.float32)
        for c, pair in enumerate(((m00, m10), (m01, m11))):
            for i in range(pieces):
                tail_scr[:, i * piece : (i + 1) * piece] = pair[0][
                    i * rest : (i + 1) * rest, body:
                ].astype(jnp.float32) + pair[1][i * rest : (i + 1) * rest, body:].astype(
                    jnp.float32
                )

            def one_tile(j, sums):
                at = pl.multiple_of(j * TILE, TILE)
                column = pl.ds(pl.multiple_of(c * half + at, TILE), TILE)
                arrived = []
                for t in range(groups):
                    where = pl.ds(pl.multiple_of(t * half + at, TILE), TILE)
                    arrived.append(
                        pair[0][:, where].astype(jnp.float32)
                        + pair[1][:, where].astype(jnp.float32)
                    )
                arrived.append(tail_scr[:, pl.ds(at, TILE)])
                tile = jnp.dot(
                    a_ref[place], w_ref[:, column], preferred_element_type=jnp.float32
                ) + jnp.concatenate(arrived, axis=0)
                hidden = res_ref[:, column].astype(jnp.float32) + gate_ref[:, column] * tile
                hid_scr[:, column] = hidden
                return sums + hidden

            sums = lax.fori_loop(0, tiles, one_tile, sums)
        mean = jnp.sum(sums, axis=1, keepdims=True) / columns

        def square_tile(j, squares):
            centered = hid_scr[:, pl.ds(pl.multiple_of(j * TILE, TILE), TILE)] - mean
            return squares + centered * centered

        squares = lax.fori_loop(
            0, 2 * tiles, square_tile, jnp.zeros((rows, TILE), jnp.float32)
        )
        variance = jnp.sum(squares, axis=1, keepdims=True) / columns
        inverse = lax.rsqrt(variance + norm_eps)

        def head_tile(j, velocity):
            column = pl.ds(pl.multiple_of(j * TILE, TILE), TILE)
            normed = (hid_scr[:, column] - mean) * inverse * (
                1.0 + scale_ref[:, column]
            ) + shift_ref[:, column]
            return velocity + lax.dot_general(
                head_ref[:, column],
                normed.astype(jnp.bfloat16),
                (((1,), (1,)), ((), ())),
                preferred_element_type=jnp.float32,
            )

        velocity = lax.fori_loop(
            0, 2 * tiles, head_tile, jnp.zeros((latent_width, rows), jnp.float32)
        )
        vel_ref[...] = velocity
        stepped = lat_ref[...] + change_ref[0] * velocity
        step_ref[...] = stepped
        hand_ref[...] = stepped.astype(jnp.bfloat16)

    small = jax.ShapeDtypeStruct((latent_width, rows), jnp.float32)
    return pl.pallas_call(
        kernel,
        in_specs=[pl.BlockSpec(memory_space=pltpu.SMEM)] + [whole()] * 12,
        out_specs=[whole()] * 3,
        out_shape=[small, small, jax.ShapeDtypeStruct(small.shape, jnp.bfloat16)],
        scratch_shapes=[
            pltpu.VMEM((rows, columns), jnp.float32),
            pltpu.VMEM((rest, half), jnp.float32),
        ],
        compiler_params=pltpu.CompilerParams(vmem_limit_bytes=16 * 1024 * 1024),
        name="finish_rows",
    )(change.reshape(1), attention, weight, *messages, residual, *modulation, head, latent)


def join_latents(rows, first_order, own_tokens, stepped, velocity, change, is_low):
    peers, latent_width, block_rows = rows.shape

    def kernel(change_ref, low_ref, rows_ref, order_ref, own_ref, step_ref, vel_ref, out_ref):
        own = own_ref[...]
        started = jnp.zeros((latent_width, block_rows), jnp.float32)
        for d in range(peers):
            same = (own == order_ref[d : d + 1, :]).astype(jnp.float32).astype(jnp.bfloat16)
            started += lax.dot_general(
                rows_ref[d], same, (((1,), (1,)), ((), ())), preferred_element_type=jnp.float32
            )
        finished = started + change_ref[0] * vel_ref[...]
        out_ref[...] = jnp.where(low_ref[0] == 1, finished, step_ref[...])

    scalar = pl.BlockSpec(memory_space=pltpu.SMEM)
    return pl.pallas_call(
        kernel,
        in_specs=[scalar, scalar] + [whole()] * 5,
        out_specs=whole(),
        out_shape=jax.ShapeDtypeStruct((latent_width, block_rows), jnp.float32),
        compiler_params=pltpu.CompilerParams(vmem_limit_bytes=16 * 1024 * 1024),
        name="join_latents",
    )(change.reshape(1), is_low.reshape(1), rows, first_order, own_tokens, stepped, velocity)


def shards(
    query_heads,
    key_heads,
    value_heads,
    residual,
    out_weight,
    mod_weight,
    head_weight,
    latent,
    timesteps,
    token_order,
):
    peers = lax.axis_size("seq")
    seq_index = lax.axis_index("seq")
    expert_index = lax.axis_index("expert")
    block_rows = query_heads.shape[2]
    model_width = residual.shape[3]
    far = peers // 2

    outgoing = pack_messages(
        query_heads[0, 0], key_heads[0, 0], value_heads[0, 0], seq_index, expert_index, peers
    )
    arrived = [None] * peers
    arrived[0] = outgoing[0]
    order = [far]
    for d in range(far - 1, 0, -1):
        order += [d, peers - d]
    for d in order:
        arrived[d] = shift(outgoing[d], "seq", d)
    order.append(0)

    orders = lax.dynamic_index_in_dim(token_order, expert_index, 0, keepdims=False)[0]
    by_device = orders.reshape(peers, block_rows)
    doubled = jnp.concatenate([by_device[::-1], by_device[::-1]], axis=0)
    slot_tokens = lax.dynamic_slice_in_dim(doubled, peers - 1 - seq_index, peers, axis=0)
    own_tokens = slot_tokens[0]
    tables = rope_tables(slot_tokens, token_order.shape[2])

    step_value = timesteps[0, 0].astype(jnp.float32)
    embedded = stamp_embedding(step_value).astype(jnp.bfloat16)
    modulation = jnp.dot(embedded[None], mod_weight[0], preferred_element_type=jnp.float32)
    modulation = [
        modulation[:, i * model_width : (i + 1) * model_width] for i in range(3)
    ]
    change = noise_level(step_value - STRIDE) - noise_level(step_value)

    gather_bits = list(range(peers.bit_length() - 2, -1, -1))
    offsets = [0]
    for bit in gather_bits:
        offsets += [offset | 1 << bit for offset in offsets]
    first_order = jnp.take(
        token_order[0, 0].reshape(peers, block_rows),
        seq_index ^ jnp.array(offsets),
        axis=0,
        mode="clip",
    )
    tables, modulation, change, first_order, own_column = lax.optimization_barrier(
        (tables, modulation, change, first_order, own_tokens[:, None])
    )

    turned_q, turned_k, values = turn_rows(arrived, tables, order)
    attended = {}
    first = 0
    for count in (3, 6, peers - 9):
        block = attend(turned_q, turned_k, values, first, count, False)
        for i in range(count):
            attended[order[first + i]] = (block, i)
        first += count

    weight = out_weight[0]
    chains = {(way, c): None for way in (1, -1) for c in (0, 1)}
    for way, c in ((1, 0), (-1, 1)):
        chains[way, c] = shift(
            add_partial(*attended[far], weight, c, None, 1280), "seq", way
        )
    for distance in range(far - 1, 0, -1):
        for way, c in ((1, 1), (-1, 0), (1, 0), (-1, 1)):
            source = attended[-way * distance % peers]
            step = 1280
            chains[way, c] = shift(
                add_partial(*source, weight, c, chains[way, c], step), "seq", way
            )
    velocity, stepped, handed = finish_rows(
        *attended[0],
        weight,
        [chains[1, 0], chains[-1, 0], chains[1, 1], chains[-1, 1]],
        residual[0, 0],
        modulation,
        head_weight[0].T,
        latent[0].T,
        change,
    )

    rows = handed[None]
    for bit in gather_bits:
        pairs = [(i, i ^ 1 << bit) for i in range(peers)]
        rows = jnp.concatenate([rows, lax.ppermute(rows, ("expert", "seq"), pairs)], axis=0)
    rows = lax.ppermute(rows, "expert", [(0, 1)])
    finished = join_latents(
        rows, first_order, own_column, stepped, velocity, change, expert_index
    )
    return (velocity.T[None, None], finished.T[None, None])


def solution(mesh):
    return jax.shard_map(
        shards,
        mesh=mesh,
        in_specs=(
            P("expert", "groups", "seq", None),
            P("expert", "groups", "seq", None),
            P("expert", "groups", "seq", None),
            P("expert", "groups", "seq", None),
            P("expert", "seq", None),
            P("expert", None, None),
            P("expert", None, None),
            P("groups", "seq", None),
            P("expert", "groups"),
            P(None, "groups", None),
        ),
        out_specs=(P("expert", "groups", "seq", None), P("expert", "groups", "seq", None)),
        check_vma=False,
    )
```
